8 devices in a mesh: rep: 1 (over z), dp: 8 (over x, y, core).
Axes of the slice: x: 2, y: 2, z: 1, core: 2. Of those that a mesh axis runs over, the one named last changes fastest.
Arguments:
- x: bfloat16 [8, 2048, 1280], P(('rep', 'dp'))
- dy: bfloat16 [8, 2048, 1280], P(('rep', 'dp'))
- w_gate: bfloat16 [2, 1280, 5120], P(None, 'dp')
- w_up: bfloat16 [2, 1280, 5120], P(None, 'dp')
- w_down: bfloat16 [2, 5120, 1280], P(None, 'dp')
- m_w_gate: float32 [2, 1280, 5120], P(None, 'dp')
- m_w_up: float32 [2, 1280, 5120], P(None, 'dp')
- m_w_down: float32 [2, 5120, 1280], P(None, 'dp')
- v_w_gate: float32 [2, 1280, 5120], P(None, 'dp')
- v_w_up: float32 [2, 1280, 5120], P(None, 'dp')
- v_w_down: float32 [2, 5120, 1280], P(None, 'dp')
Outputs:
- output 1: bfloat16 [2, 1280, 5120], P('rep', 'dp')
- output 2: bfloat16 [2, 1280, 5120], P('rep', 'dp')
- output 3: bfloat16 [2, 5120, 1280], P('rep', 'dp')
- output 4: float32 [2, 1280, 5120], P('rep', 'dp')
- output 5: float32 [2, 1280, 5120], P('rep', 'dp')
- output 6: float32 [2, 5120, 1280], P('rep', 'dp')
- output 7: float32 [2, 1280, 5120], P('rep', 'dp')
- output 8: float32 [2, 1280, 5120], P('rep', 'dp')
- output 9: float32 [2, 5120, 1280], P('rep', 'dp')
All inputs are finite; a program needn't handle non-finite values.
Results may differ from the reference program's by a relative error of at most 0.022.
Values are sent between devices in bfloat16 or wider.
A program may use at most 2 GiB of HBM per device.

```python
import jax
import jax.numpy as jnp
from jax import lax

SEQUENCES = 8
TOKENS = 2048
D = 1280
FF = 5120
LAYERS = 2
NAMES = ("w_gate", "w_up", "w_down")
SHAPES = {"w_gate": (LAYERS, D, FF), "w_up": (LAYERS, D, FF), "w_down": (LAYERS, FF, D)}


def bump(key, n, height):
    away = (jnp.arange(n, dtype=jnp.int32) - jax.random.randint(key, (), 0, n, jnp.int32)) % n
    return jnp.where(away < n // 8, height, 1.0)


def together(key, own, strength):
    shared = jax.random.normal(key, own.shape[1:], jnp.float32)
    return (own + strength * shared) * lax.rsqrt(1 + strength * strength)


def setup_inputs(seed: int = 0, part: int = 0) -> dict:
    kx, kdy, ka, kb, kz, kf, kh, kl, *keys = jax.random.split(jax.random.key(seed), 8 + 3 * len(NAMES))
    kx, kdy, ka, kb = (jax.random.fold_in(k, part) for k in (kx, kdy, ka, kb))
    kw, km, kv = (keys[i::3] for i in range(3))
    shape = (SEQUENCES, TOKENS, D)
    much_x, much_dy = jax.random.uniform(kz, (2,), jnp.float32, 0.0, 1.0)
    loud = 2.0 ** jax.random.uniform(jax.random.fold_in(kz, 1), (), jnp.float32, -1.0, 2.0)
    layers = 2.0 ** jax.random.uniform(kl, (LAYERS, 1, 1), jnp.float32, -1.0, 1.0)
    x = together(ka, jax.random.normal(kx, shape, jnp.float32), much_x) * bump(kf, D, 4.0)
    dy = together(kb, jax.random.normal(kdy, shape, jnp.float32), much_dy)
    drawn = {"x": x.astype(jnp.bfloat16), "dy": (loud * dy * (SEQUENCES * TOKENS) ** -0.5).astype(jnp.bfloat16)}
    for key, name in zip(kw, NAMES, strict=True):
        w = jax.random.normal(key, SHAPES[name], jnp.float32) * SHAPES[name][1] ** -0.5
        drawn[name] = (w * {"w_gate": 1.0, "w_up": bump(kh, FF, 4.0), "w_down": layers}[name]).astype(jnp.bfloat16)
    for key, name in zip(km, NAMES, strict=True):
        drawn[f"m_{name}"] = 0.1 * jax.random.normal(key, SHAPES[name], jnp.float32)
    for key, name in zip(kv, NAMES, strict=True):
        drawn[f"v_{name}"] = jax.random.uniform(key, SHAPES[name], jnp.float32, 0.005, 0.015)
    return drawn


def matmul(a, w):
    return jnp.dot(a, w, preferred_element_type=jnp.float32).astype(jnp.bfloat16)


def normed(h):
    wide = h.astype(jnp.float32)
    scale = lax.rsqrt(jnp.mean(wide**2, -1, keepdims=True) + 1e-6)
    return (wide * scale).astype(jnp.bfloat16)


def layer(h, w):
    a = normed(h)
    gate = jnp.dot(a, w["w_gate"], preferred_element_type=jnp.float32)
    up = jnp.dot(a, w["w_up"], preferred_element_type=jnp.float32)
    return h + matmul((jax.nn.silu(gate) * up).astype(jnp.bfloat16), w["w_down"])


def adamw(w, m, v, g):
    m = 0.9 * m + 0.1 * g
    v = 0.95 * v + 0.05 * g * g
    step = m * lax.rsqrt(v + 1e-8) + 0.1 * w
    return (w - 0.02 * step).astype(jnp.bfloat16), m, v


def clipped(gradients, sum_of_squares, count):
    factor = jnp.minimum(1.0, 0.5 * lax.rsqrt(sum_of_squares / count + 1e-30))
    return [g * factor for g in gradients]


def stack(weights, h):
    return lax.scan(lambda h, w: (layer(h, w), None), h, weights)[0]


def reference(x, dy, w_gate, w_up, w_down, m_w_gate, m_w_up, m_w_down, v_w_gate, v_w_up, v_w_down):
    weights = dict(zip(NAMES, (w_gate, w_up, w_down), strict=True))

    def take(so_far, sequence):
        h, by_y = sequence
        _, back = jax.vjp(lambda w: stack(w, h), weights)
        return jax.tree.map(lambda total, term: total + term.astype(jnp.float32), so_far, back(by_y)[0]), None

    none_yet = {name: jnp.zeros(w.shape, jnp.float32) for name, w in weights.items()}
    by_weights, _ = lax.scan(take, none_yet, (x, dy))
    gradients = [by_weights[name].astype(jnp.bfloat16).astype(jnp.float32) for name in NAMES]
    gradients = clipped(gradients, sum(jnp.sum(g * g) for g in gradients), sum(g.size for g in gradients))
    new = [
        adamw(w.astype(jnp.float32), m, v, g)
        for w, m, v, g in zip((w_gate, w_up, w_down), (m_w_gate, m_w_up, m_w_down), (v_w_gate, v_w_up, v_w_down), gradients, strict=True)
    ]
    return tuple(one[which] for which in range(3) for one in new)
```

```python
import functools

import jax
import jax.numpy as jnp
from jax import lax
from jax.experimental import pallas as pl
from jax.experimental.pallas import tpu as pltpu
from jax.sharding import PartitionSpec as P

F32, BF16 = jnp.float32, jnp.bfloat16
X, Y, C = (1, 0, 0), (0, 1, 0), (0, 0, 1)
DIAGONAL = (1, 1, 0)
MESH = pl.DeviceIdType.MESH
ANY = pl.BlockSpec(memory_space=pl.ANY)
VMEM_LIMIT = 61 * 2**20


def dot(a, b, ca, cb):
    return lax.dot_general(a, b, (((ca,), (cb,)), ((), ())), preferred_element_type=F32)


def place(flip):
    index = lax.axis_index("dp")
    x, y, core = index // 4, index // 2 % 2, index % 2
    return (x + flip[0]) % 2 * 4 + (y + flip[1]) % 2 * 2 + (core + flip[2]) % 2


def remote(src, dst, send, receive, flip):
    return pltpu.make_async_remote_copy(
        src_ref=src, dst_ref=dst, send_sem=send, recv_sem=receive, device_id={"dp": place(flip)}, device_id_type=MESH
    )


def greet():
    barrier = pltpu.get_barrier_semaphore()
    for flip in (X, Y, C):
        pl.semaphore_signal(barrier, inc=1, device_id={"dp": place(flip)}, device_id_type=MESH)
    pl.semaphore_wait(barrier, 3)


class Gather:
    def __init__(self, shard, middle):
        self.inputs, self.middle = [shard], middle
        rows, cols = shard.shape
        self.outputs = [jax.ShapeDtypeStruct((8 * rows, cols), BF16)]
        self.scratch = [pltpu.VMEM((rows, cols), BF16), pltpu.SemaphoreType.DMA((2,)), pltpu.SemaphoreType.DMA((13,)), pltpu.SemaphoreType.DMA((13,))]

    def bind(self, refs_in, refs_out, scratch):
        (self.shard,), (self.full,), (self.held, self.local, self.send, self.receive) = refs_in, refs_out, scratch
        rows = self.shard.shape[0]
        half = rows // 2

        def part(flip, first, count):
            return self.full.at[pl.ds(pl.multiple_of(place(flip) * rows, 16) + first, count)]

        def copy(number, flip, of, first, count):
            src = self.shard.at[pl.ds(first, count)] if of is None else part(of, first, count)
            return remote(src, part(of or (0, 0, 0), first, count), self.send.at[number], self.receive.at[number], flip)

        self.xa, self.xb = copy(0, X, None, 0, half), copy(1, X, None, half, half)
        self.yb, self.ya = copy(2, Y, None, half, half), copy(3, Y, None, 0, half)
        self.low, self.high = copy(4, Y, X, 0, half), copy(5, X, Y, half, half)
        self.own = copy(6, C, None, 0, rows)
        self.cxa, self.cxb = copy(7, C, X, 0, half), copy(8, C, X, half, half)
        self.cyb, self.cya = copy(9, C, Y, half, half), copy(10, C, Y, 0, half)
        self.clow, self.chigh = copy(11, C, DIAGONAL, 0, half), copy(12, C, DIAGONAL, half, half)
        self.load = pltpu.make_async_copy(self.shard, self.held, self.local.at[0])
        self.store = pltpu.make_async_copy(self.held, part((0, 0, 0), 0, rows), self.local.at[1])

    def start(self):
        for one in (self.xa, self.yb, self.xb, self.ya, self.own, self.load):
            one.start()

    def relay(self):
        self.xa.wait_recv()
        self.low.start()
        self.cxa.start()
        self.yb.wait_recv()
        self.high.start()
        self.cyb.start()
        self.load.wait()
        self.store.start()

    def finish(self):
        self.xb.wait_recv()
        self.cxb.start()
        self.ya.wait_recv()
        self.cya.start()
        self.low.wait_recv()
        self.clow.start()
        self.high.wait_recv()
        self.chigh.start()
        for one in (self.own, self.cxa, self.cyb, self.cxb, self.cya, self.clow, self.chigh):
            one.wait_recv()
        for one in (self.xa, self.xb, self.yb, self.ya, self.low, self.high):
            one.wait_send()
        for one in (self.own, self.cxa, self.cyb, self.cxb, self.cya, self.clow, self.chigh):
            one.wait_send()
        self.store.wait()


class Hop:
    def __init__(self, array, left, right):
        self.inputs, self.flips, self.middle = [array], (left, right), None
        self.outputs = [jax.ShapeDtypeStruct(array.shape, array.dtype)]
        self.scratch = [pltpu.SemaphoreType.DMA((2,)), pltpu.SemaphoreType.DMA((2,))]

    def bind(self, refs_in, refs_out, scratch):
        (src,), (dst,), (send, receive) = refs_in, refs_out, scratch
        half = src.shape[1] // 2
        self.copies = [
            remote(src.at[:, pl.ds(i * half, half)], dst.at[:, pl.ds(i * half, half)], send.at[i], receive.at[i], flip)
            for i, flip in enumerate(self.flips)
        ]

    def start(self):
        for one in self.copies:
            one.start()

    def finish(self):
        for one in self.copies:
            one.wait_recv()
        for one in self.copies:
            one.wait_send()


def run(number, steps, compute, ins, outs, comms, scratch=(), flops=0):
    counts = [len(ins)] + [len(c.inputs) for c in comms] + [len(outs)] + [len(c.outputs) for c in comms]
    counts += [len(scratch)] + [len(c.scratch) for c in comms]

    def kernel(*refs):
        refs, groups = list(refs), []
        for count in counts:
            groups.append(refs[:count])
            refs = refs[count:]
        k = len(comms) + 1
        g_in, g_out, g_scratch = groups[:k], groups[k : 2 * k], groups[2 * k :]
        for c, *bound in zip(comms, g_in[1:], g_out[1:], g_scratch[1:]):
            c.bind(*bound)
        step = pl.program_id(0)

        @pl.when(step == 0)
        def _():
            greet()
            for c in comms:
                c.start()

        for c in comms:
            if c.middle is not None:
                pl.when(step == c.middle)(c.relay)
        if compute is not None:
            compute(step, g_in[0], g_out[0], g_scratch[0])

        @pl.when(step == steps - 1)
        def _():
            for c in comms:
                c.finish()

    out = pl.pallas_call(
        kernel,
        grid=(steps,),
        in_specs=[spec for _, spec in ins] + [ANY for c in comms for _ in c.inputs],
        out_specs=[spec for _, spec in outs] + [ANY for c in comms for _ in c.outputs],
        out_shape=[shape for shape, _ in outs] + [shape for c in comms for shape in c.outputs],
        scratch_shapes=list(scratch) + [s for c in comms for s in c.scratch],
        compiler_params=pltpu.CompilerParams(
            collective_id=number, has_side_effects=True, vmem_limit_bytes=VMEM_LIMIT, dimension_semantics=("arbitrary",)
        ),
        cost_estimate=pl.CostEstimate(flops=flops or 10**9, bytes_accessed=5 * 10**7, transcendentals=0),
        name=f"k{number}",
    )(*[a for a, _ in ins], *[a for c in comms for a in c.inputs])
    return out


def shape(rows, cols, dtype=BF16):
    return jax.ShapeDtypeStruct((rows, cols), dtype)


def norm_rows(wide):
    scale = lax.rsqrt(jnp.mean(wide * wide, -1, keepdims=True) + 1e-6)
    return scale, (wide * scale).astype(BF16)


def k_norm(number, h, comms):
    tokens, d = h.shape
    rows = tokens // 4
    block = pl.BlockSpec((rows, d), lambda i: (i, 0))

    def compute(step, ins, outs, _):
        outs[0][...] = norm_rows(ins[0][...].astype(F32))[1]

    return run(number, 4, compute, [(h, block)], [(shape(tokens, d), block)], comms)


def k_gate(number, a, w, comms):
    (tokens, d), ff = a.shape, w.shape[1]
    m, n = tokens // 2, ff // 4

    def compute(step, ins, outs, _):
        outs[0][...] = dot(ins[0][...], ins[1][...], 1, 0)

    return run(
        number, 8, compute,
        [(a, pl.BlockSpec((m, d), lambda i: (i // 4, 0))), (w, pl.BlockSpec((d, n), lambda i: (0, i % 4)))],
        [(shape(tokens, ff, F32), pl.BlockSpec((m, n), lambda i: (i // 4, i % 4)))],
        comms,
    )


def k_up(number, a, w, gate, comms):
    (tokens, d), ff = a.shape, w.shape[1]
    m, n = tokens // 2, ff // 4
    tile = pl.BlockSpec((m, n), lambda i: (i // 4, i % 4))

    def compute(step, ins, outs, _):
        up = dot(ins[0][...], ins[1][...], 1, 0)
        outs[0][...] = up
        outs[1][...] = (jax.nn.silu(ins[2][...]) * up).astype(BF16)

    return run(
        number, 8, compute,
        [(a, pl.BlockSpec((m, d), lambda i: (i // 4, 0))), (w, pl.BlockSpec((d, n), lambda i: (0, i % 4))), (gate, tile)],
        [(shape(tokens, ff, F32), tile), (shape(tokens, ff), tile)],
        comms,
    )


def k_down(number, s, w, h, comms):
    (tokens, ff), d = s.shape, w.shape[1]
    m = tokens // 4
    rows = pl.BlockSpec((m, d), lambda i: (i, 0))

    def compute(step, ins, outs, _):
        new = ins[2][...] + dot(ins[0][...], ins[1][...], 1, 0).astype(BF16)
        outs[0][...] = new
        outs[1][...] = norm_rows(new.astype(F32))[1]

    return run(
        number, 4, compute,
        [(s, pl.BlockSpec((m, ff), lambda i: (i, 0))), (w, pl.BlockSpec((ff, d), lambda i: (0, 0), pipeline_mode=pl.Buffered(1))), (h, rows)],
        [(shape(tokens, d), rows), (shape(tokens, d), rows)],
        comms,
    )


def k_back_gated(number, d_out, w, gate, up, comms):
    (tokens, d), ff = d_out.shape, w.shape[0]
    m, n = tokens // 2, ff // 4
    tile = pl.BlockSpec((m, n), lambda i: (i // 4, i % 4))

    def compute(step, ins, outs, _):
        ds = dot(ins[0][...], ins[1][...], 1, 1).astype(BF16).astype(F32)
        g, u = ins[2][...], ins[3][...]
        sig = jax.nn.sigmoid(g)
        outs[0][...] = (ds * u * (sig * (1 + g * (1 - sig)))).astype(BF16)
        outs[1][...] = (ds * (g * sig)).astype(BF16)

    return run(
        number, 8, compute,
        [(d_out, pl.BlockSpec((m, d), lambda i: (i // 4, 0))), (w, pl.BlockSpec((n, d), lambda i: (i % 4, 0))), (gate, tile), (up, tile)],
        [(shape(tokens, ff), tile), (shape(tokens, ff), tile)],
        comms,
    )


def k_back_in(number, d_gate, w, comms):
    (tokens, ff), d = d_gate.shape, w.shape[0]
    m = tokens // 4
    rows = pl.BlockSpec((m, d), lambda i: (i, 0))

    def compute(step, ins, outs, _):
        outs[0][...] = dot(ins[0][...], ins[1][...], 1, 1).astype(BF16)

    return run(
        number, 4, compute,
        [(d_gate, pl.BlockSpec((m, ff), lambda i: (i, 0))), (w, pl.BlockSpec((d, ff), lambda i: (0, 0), pipeline_mode=pl.Buffered(1)))],
        [(shape(tokens, d), rows)],
        comms,
    )


def k_back_norm(number, d_up, w, other, h, d_out, comms):
    (tokens, ff), d = d_up.shape, w.shape[0]
    m = tokens // 4
    rows = pl.BlockSpec((m, d), lambda i: (i, 0))

    def compute(step, ins, outs, _):
        da = (dot(ins[0][...], ins[1][...], 1, 1).astype(BF16) + ins[2][...]).astype(F32)
        wide = ins[3][...].astype(F32)
        scale, _ = norm_rows(wide)
        inner = jnp.sum(da * wide, -1, keepdims=True) / d
        dh = da * scale - wide * (scale * scale * scale * inner)
        outs[0][...] = ins[4][...] + dh.astype(BF16)

    return run(
        number, 4, compute,
        [(d_up, pl.BlockSpec((m, ff), lambda i: (i, 0))), (w, pl.BlockSpec((d, ff), lambda i: (0, 0), pipeline_mode=pl.Buffered(1))), (other, rows), (h, rows), (d_out, rows)],
        [(shape(tokens, d), rows)],
        comms,
    )


def exchange_scratch(rows, cols):
    return [pltpu.VMEM((4, rows, cols), BF16)] * 2 + [pltpu.SemaphoreType.DMA((4,))] * 2


def exchange(step, theirs, tile, product, scratch, write):
    made, came, send, receive = scratch

    def copy(i):
        return remote(made.at[i], came.at[i], send.at[i], receive.at[i], C)

    for i in range(4):
        pl.when(step == i + 1)(lambda i=i: copy(i).start())

    @pl.when(step < 4)
    def _():
        made[step] = product().astype(BF16)

    for i in range(4):

        @pl.when(step == i + 4)
        def _(i=i):
            total = product()
            copy(i).wait_recv()
            write(i, total + came[i].astype(F32))
            if i == 3:
                for k in range(4):
                    copy(k).wait_send()


def k_gradient_in(number, a_split, d_gate, comms):
    (tokens, d), ff = a_split.shape, d_gate.shape[1]
    rows, n = d // 8, ff // 4
    out = pl.BlockSpec((2 * rows, n), lambda i: (0, jnp.maximum(i - 4, 0)))

    def compute(step, ins, outs, scratch):
        def write(i, total):
            self, y, x, xy = (total[k * rows : (k + 1) * rows] for k in range(4))
            near, far = (x, y) if i < 2 else (y, x)
            outs[0][:rows, :] = near.astype(BF16)
            outs[0][rows:, :] = xy.astype(BF16)
            outs[1][:rows, :] = self
            outs[1][rows:, :] = far

        exchange(step, None, None, lambda: dot(ins[0][...], ins[1][...], 0, 0), scratch, write)

    return run(
        number, 8, compute,
        [(a_split, pl.BlockSpec((tokens, d // 2), lambda i: (0, i // 4))), (d_gate, pl.BlockSpec((tokens, n), lambda i: (0, i % 4)))],
        [(shape(2 * rows, ff), out), (shape(2 * rows, ff, F32), out)],
        comms,
        exchange_scratch(4 * rows, n),
    )


def k_gradient_down(number, s, d_out, comms):
    (tokens, ff), d = s.shape, d_out.shape[1]
    rows, half = ff // 8, d // 2
    whole = pl.BlockSpec((2 * rows, d), lambda i: (0, 0), pipeline_mode=pl.Buffered(1))

    def block(i):
        return 0, place((i // 2 % 2, i % 2, 1 - i // 4))

    def compute(step, ins, outs, scratch):
        send, keep = outs

        def write(i, total):
            if i == 0:
                keep[:rows, :] = total
            elif i == 1:
                keep[rows:, :half] = total[:, :half]
                send[:rows, half:] = total[:, half:].astype(BF16)
            elif i == 2:
                send[:rows, :half] = total[:, :half].astype(BF16)
                keep[rows:, half:] = total[:, half:]
            else:
                send[rows:, :] = total.astype(BF16)

        exchange(step, None, None, lambda: dot(ins[0][...], ins[1][...], 0, 0), scratch, write)

    return run(
        number, 8, compute,
        [(s, pl.BlockSpec((tokens, rows), block)), (d_out, pl.BlockSpec((tokens, d), lambda i: (0, 0), pipeline_mode=pl.Buffered(1)))],
        [(shape(2 * rows, d), whole), (shape(2 * rows, d, F32), whole)],
        comms,
        exchange_scratch(rows, d),
    )


def split_columns(a):
    width = a.shape[1] // 8
    flips = [(i // 2 % 2, i % 2, 1 - i // 4) for i in range(8)]
    return jnp.concatenate([lax.dynamic_slice(a, (0, place(f) * width), (a.shape[0], width)) for f in flips], 1)


def added(keep, got):
    total = keep + got.astype(F32)
    rows = keep.shape[0] // 2
    return total[rows:].astype(BF16), total[:rows]


def last(keep, got):
    g = (keep + got.astype(F32)).astype(BF16)
    wide = g.astype(F32)
    return g, jnp.sum(wide * wide)


def adamw(w, m, v, g):
    m = 0.9 * m + 0.1 * g
    v = 0.95 * v + 0.05 * g * g
    step = m * lax.rsqrt(v + 1e-8) + 0.1 * w
    return (w - 0.02 * step).astype(BF16), m, v


def solution(mesh):
    def step(x, dy, *arrays):
        weights, ms, vs = (arrays[i : i + 3] for i in (0, 3, 6))
        h0, dy = x[0], dy[0]
        (g0, g1), (u0, u1), (d0, d1) = ((w[0], w[1]) for w in weights)

        a0, wg0 = k_norm(0, h0, [Gather(g0, 1)])
        gate0, wu0 = k_gate(1, a0, wg0, [Gather(u0, 4)])
        up0, s0, wd0 = k_up(2, a0, wu0, gate0, [Gather(d0, 4)])
        h1, a1, wg1 = k_down(3, s0, wd0, h0, [Gather(g1, 2)])
        gate1, wu1 = k_gate(4, a1, wg1, [Gather(u1, 4)])
        up1, s1, wd1 = k_up(5, a1, wu1, gate1, [Gather(d1, 4)])
        a0s, a1s = split_columns(a0), split_columns(a1)

        done, total = {}, 0.0

        def finish(name, keep, got):
            nonlocal total
            done[name], square = last(keep, got)
            total += square

        d1_send, d1_keep = k_gradient_down(6, s1, dy, [])
        dgate1, dup1, got = k_back_gated(7, dy, wd1, gate1, up1, [Hop(d1_send, X, Y)])
        d1_send, d1_keep = added(d1_keep, got)
        g1_send, g1_keep, got = k_gradient_in(8, a1s, dgate1, [Hop(d1_send, Y, X)])
        finish("d1", d1_keep, got)
        u1_send, u1_keep, got = k_gradient_in(9, a1s, dup1, [Hop(g1_send, X, Y)])
        g1_send, g1_keep = added(g1_keep, got)
        part, got = k_back_in(10, dgate1, wg1, [Hop(u1_send, X, Y)])
        u1_send, u1_keep = added(u1_keep, got)
        dh1, got_g, got_u = k_back_norm(11, dup1, wu1, part, h1, dy, [Hop(g1_send, Y, X), Hop(u1_send, Y, X)])
        finish("g1", g1_keep, got_g)
        finish("u1", u1_keep, got_u)
        d0_send, d0_keep = k_gradient_down(12, s0, dh1, [])
        dgate0, dup0, got = k_back_gated(13, dh1, wd0, gate0, up0, [Hop(d0_send, X, Y)])
        d0_send, d0_keep = added(d0_keep, got)
        g0_send, g0_keep, got = k_gradient_in(14, a0s, dgate0, [Hop(d0_send, Y, X)])
        finish("d0", d0_keep, got)
        u0_send, u0_keep, got = k_gradient_in(15, a0s, dup0, [Hop(g0_send, X, Y)])
        g0_send, g0_keep = added(g0_keep, got)
        got_g, got = run(16, 1, None, [], [], [Hop(g0_send, Y, X), Hop(u0_send, X, Y)])
        finish("g0", g0_keep, got_g)
        u0_send, u0_keep = added(u0_keep, got)
        (got,) = run(17, 1, None, [], [], [Hop(u0_send, Y, X)])
        finish("u0", u0_keep, got)

        for bit in (1, 2, 4):
            total = total + lax.ppermute(total, "dp", [(i, i ^ bit) for i in range(8)])
        count = 8 * sum(g.size for g in done.values())
        factor = jnp.minimum(1.0, 0.5 * lax.rsqrt(total / count + 1e-30))
        new = []
        for i, name in enumerate("gud"):
            g = jnp.stack([done[name + "0"], done[name + "1"]]).astype(F32) * factor
            new.append(adamw(weights[i].astype(F32), ms[i], vs[i], g))
        return tuple(one[which] for which in range(3) for one in new)

    states, cut = P(("rep", "dp"), None, None), P(None, "dp", None)
    return jax.shard_map(
        step,
        mesh=mesh,
        in_specs=(states, states) + (cut,) * 9,
        out_specs=(P("rep", "dp", None),) * 9,
        check_vma=False,
    )
```

```python
import jax
import jax.numpy as jnp
from jax import lax
from jax.experimental import pallas as pl
from jax.experimental.pallas import tpu as pltpu
from jax.sharding import PartitionSpec as P

F32, BF16 = jnp.float32, jnp.bfloat16
X, Y, C = (1, 0, 0), (0, 1, 0), (0, 0, 1)
DIAGONAL = (1, 1, 0)
MESH = pl.DeviceIdType.MESH
ANY = pl.BlockSpec(memory_space=pl.ANY)
VMEM_LIMIT = 63 * 2**20


def dot(a, b, ca, cb):
    return lax.dot_general(a, b, (((ca,), (cb,)), ((), ())), preferred_element_type=F32)


def place(flip):
    index = lax.axis_index("dp")
    x, y, core = index // 4, index // 2 % 2, index % 2
    return (x + flip[0]) % 2 * 4 + (y + flip[1]) % 2 * 2 + (core + flip[2]) % 2


def remote(src, dst, send, receive, flip):
    return pltpu.make_async_remote_copy(
        src_ref=src, dst_ref=dst, send_sem=send, recv_sem=receive, device_id={"dp": place(flip)}, device_id_type=MESH
    )


def greet():
    barrier = pltpu.get_barrier_semaphore()
    for flip in (X, Y, C):
        pl.semaphore_signal(barrier, inc=1, device_id={"dp": place(flip)}, device_id_type=MESH)
    pl.semaphore_wait(barrier, 3)


class Gather:
    def __init__(self, shard, middle):
        self.inputs, self.middle = [shard], middle
        rows, cols = shard.shape
        self.outputs = [jax.ShapeDtypeStruct((8 * rows, cols), BF16)]
        self.scratch = [pltpu.VMEM((rows, cols), BF16), pltpu.SemaphoreType.DMA((2,)), pltpu.SemaphoreType.DMA((13,)), pltpu.SemaphoreType.DMA((13,))]

    def bind(self, refs_in, refs_out, scratch):
        (self.shard,), (self.full,), (self.held, self.local, self.send, self.receive) = refs_in, refs_out, scratch
        rows = self.shard.shape[0]
        half = rows // 2

        def part(flip, first, count):
            return self.full.at[pl.ds(pl.multiple_of(place(flip) * rows, 16) + first, count)]

        def copy(number, flip, of, first, count):
            src = self.shard.at[pl.ds(first, count)] if of is None else part(of, first, count)
            return remote(src, part(of or (0, 0, 0), first, count), self.send.at[number], self.receive.at[number], flip)

        self.xa, self.xb = copy(0, X, None, 0, half), copy(1, X, None, half, half)
        self.yb, self.ya = copy(2, Y, None, half, half), copy(3, Y, None, 0, half)
        self.low, self.high = copy(4, Y, X, 0, half), copy(5, X, Y, half, half)
        self.own = copy(6, C, None, 0, rows)
        self.cxa, self.cxb = copy(7, C, X, 0, half), copy(8, C, X, half, half)
        self.cyb, self.cya = copy(9, C, Y, half, half), copy(10, C, Y, 0, half)
        self.clow, self.chigh = copy(11, C, DIAGONAL, 0, half), copy(12, C, DIAGONAL, half, half)
        self.load = pltpu.make_async_copy(self.shard, self.held, self.local.at[0])
        self.store = pltpu.make_async_copy(self.held, part((0, 0, 0), 0, rows), self.local.at[1])

    def start(self):
        for one in (self.xa, self.yb, self.xb, self.ya, self.own, self.load):
            one.start()

    def relay(self):
        self.xa.wait_recv()
        self.low.start()
        self.cxa.start()
        self.yb.wait_recv()
        self.high.start()
        self.cyb.start()
        self.load.wait()
        self.store.start()

    def finish(self):
        self.xb.wait_recv()
        self.cxb.start()
        self.ya.wait_recv()
        self.cya.start()
        self.low.wait_recv()
        self.clow.start()
        self.high.wait_recv()
        self.chigh.start()
        for one in (self.own, self.cxa, self.cyb, self.cxb, self.cya, self.clow, self.chigh):
            one.wait_recv()
        for one in (self.xa, self.xb, self.yb, self.ya, self.low, self.high):
            one.wait_send()
        for one in (self.own, self.cxa, self.cyb, self.cxb, self.cya, self.clow, self.chigh):
            one.wait_send()
        self.store.wait()


class Hop:
    def __init__(self, array, left, right):
        self.inputs, self.flips, self.middle = [array], (left, right), None
        self.outputs = [jax.ShapeDtypeStruct(array.shape, array.dtype)]
        self.scratch = [pltpu.SemaphoreType.DMA((2,)), pltpu.SemaphoreType.DMA((2,))]

    def bind(self, refs_in, refs_out, scratch):
        (src,), (dst,), (send, receive) = refs_in, refs_out, scratch
        half = src.shape[1] // 2
        self.copies = [
            remote(src.at[:, pl.ds(i * half, half)], dst.at[:, pl.ds(i * half, half)], send.at[i], receive.at[i], flip)
            for i, flip in enumerate(self.flips)
        ]

    def start(self):
        for one in self.copies:
            one.start()

    def finish(self):
        for one in self.copies:
            one.wait_recv()
        for one in self.copies:
            one.wait_send()


class AddHop:
    def __init__(self, keep, got, left, right, middle):
        self.inputs, self.flips, self.middle = [keep, got], (left, right), middle
        rows, cols = keep.shape[0] // 2, keep.shape[1]
        self.outputs = [jax.ShapeDtypeStruct((rows, cols), F32), jax.ShapeDtypeStruct((rows, cols), BF16)]
        self.scratch = [pltpu.VMEM(keep.shape, F32), pltpu.VMEM(got.shape, BF16), pltpu.VMEM((rows, cols), BF16), pltpu.SemaphoreType.DMA((3,))]
        self.scratch += [pltpu.SemaphoreType.DMA((2,)), pltpu.SemaphoreType.DMA((2,))]

    def bind(self, refs_in, refs_out, scratch):
        (keep, got), (stay, dst), (self.sum, self.came, self.out, local, send, receive) = refs_in, refs_out, scratch
        self.rows, half = dst.shape[0], dst.shape[1] // 2
        self.loads = [pltpu.make_async_copy(keep, self.sum, local.at[0]), pltpu.make_async_copy(got, self.came, local.at[1])]
        self.store = pltpu.make_async_copy(self.sum.at[pl.ds(0, self.rows)], stay, local.at[2])
        self.copies = [
            remote(self.out.at[:, pl.ds(i * half, half)], dst.at[:, pl.ds(i * half, half)], send.at[i], receive.at[i], flip)
            for i, flip in enumerate(self.flips)
        ]

    def start(self):
        for one in self.loads:
            one.start()

    def relay(self):
        for one in self.loads:
            one.wait()
        rows = self.rows
        self.out[...] = (self.sum[rows:, :] + self.came[rows:, :].astype(F32)).astype(BF16)
        self.sum[:rows, :] = self.sum[:rows, :] + self.came[:rows, :].astype(F32)
        self.store.start()
        for one in self.copies:
            one.start()

    def finish(self):
        for one in self.copies:
            one.wait_recv()
        for one in self.copies:
            one.wait_send()
        self.store.wait()


def run(number, steps, compute, ins, outs, comms, scratch=(), flops=0, sides=()):
    sides = [side(steps) for side in sides]
    counts = [len(ins)] + [len(s[0]) for s in sides] + [len(c.inputs) for c in comms]
    counts += [len(outs)] + [len(s[1]) for s in sides] + [len(c.outputs) for c in comms]
    counts += [len(scratch)] + [len(c.scratch) for c in comms]

    def kernel(*refs):
        refs, groups = list(refs), []
        for count in counts:
            groups.append(refs[:count])
            refs = refs[count:]
        n, k = len(sides), len(sides) + len(comms) + 1
        g_in, g_out, g_scratch = groups[:k], groups[k : 2 * k], groups[2 * k :]
        for c, *bound in zip(comms, g_in[1 + n :], g_out[1 + n :], g_scratch[1:]):
            c.bind(*bound)
        step = pl.program_id(0)

        @pl.when(step == 0)
        def _():
            greet()
            for c in comms:
                c.start()

        for c in comms:
            if c.middle is not None:
                pl.when(step == c.middle)(c.relay)
        if compute is not None:
            compute(step, g_in[0], g_out[0], g_scratch[0])
        for s, s_in, s_out in zip(sides, g_in[1:], g_out[1:]):
            s[2](s_in, s_out)

        @pl.when(step == steps - 1)
        def _():
            for c in comms:
                c.finish()

    ins = list(ins) + [one for s in sides for one in s[0]]
    outs = list(outs) + [one for s in sides for one in s[1]]
    return pl.pallas_call(
        kernel,
        grid=(steps,),
        in_specs=[spec for _, spec in ins] + [ANY for c in comms for _ in c.inputs],
        out_specs=[spec for _, spec in outs] + [ANY for c in comms for _ in c.outputs],
        out_shape=[shape for shape, _ in outs] + [shape for c in comms for shape in c.outputs],
        scratch_shapes=list(scratch) + [s for c in comms for s in c.scratch],
        compiler_params=pltpu.CompilerParams(
            collective_id=number, has_side_effects=True, vmem_limit_bytes=VMEM_LIMIT, dimension_semantics=("arbitrary",)
        ),
        cost_estimate=pl.CostEstimate(flops=flops or 10**9, bytes_accessed=5 * 10**7, transcendentals=0),
        name=f"k{number}",
    )(*[a for a, _ in ins], *[a for c in comms for a in c.inputs])


def blocks(rows, cols, steps):
    n = min(steps, 8)
    per = steps // n
    if rows % (16 * n) == 0:
        return tuple(pl.BlockSpec((rows // n, cols), lambda i, k=k: (i // per + k * n, 0)) for k in (0, 1)) + (n, pl.BlockSpec((8, cols), lambda i: (i // per, 0)))
    return tuple(pl.BlockSpec((rows, cols // n), lambda i, k=k: (k, i // per)) for k in (0, 1)) + (1, pl.BlockSpec((8, cols // n), lambda i: (0, i // per)))


def side_last(keep, got):
    rows, cols = keep.shape

    def side(steps):
        low, _, n, sums = blocks(rows, cols, steps)

        def compute(ins, outs):
            g = (ins[0][...] + ins[1][...].astype(F32)).astype(BF16)
            outs[0][...] = g
            wide = g.astype(F32)
            outs[1][...] = jnp.sum((wide * wide).reshape(-1, 8, wide.shape[1]), 0)

        return [(keep, low), (got, low)], [(shape(rows, cols), low), (shape(8 * n, cols, F32), sums)], compute

    return side


def shape(rows, cols, dtype=BF16):
    return jax.ShapeDtypeStruct((rows, cols), dtype)


def norm_rows(wide):
    scale = lax.rsqrt(jnp.mean(wide * wide, -1, keepdims=True) + 1e-6)
    return scale, (wide * scale).astype(BF16)


def choose(step, chosen):
    width = chosen.shape[1] // 8

    @pl.when(step == 0)
    def _():
        away = lax.broadcasted_iota(jnp.int32, (chosen.shape[0], width), 0) - lax.broadcasted_iota(jnp.int32, (chosen.shape[0], width), 1)
        for i in range(8):
            chosen[:, i * width : (i + 1) * width] = jnp.where(away == place((i // 2 % 2, i % 2, 1 - i // 4)) * width, 1.0, 0.0).astype(BF16)


def k_norm(number, h, comms):
    tokens, d = h.shape
    rows = tokens // 4
    block = pl.BlockSpec((rows, d), lambda i: (i, 0))

    def compute(step, ins, outs, scratch):
        choose(step, scratch[0])
        a = norm_rows(ins[0][...].astype(F32))[1]
        outs[0][...] = a
        outs[1][...] = dot(a, scratch[0][...], 1, 0).astype(BF16)

    return run(number, 4, compute, [(h, block)], [(shape(tokens, d), block)] * 2, comms, [pltpu.VMEM((d, d), BF16)])


def k_gate(number, a, w, comms):
    (tokens, d), ff = a.shape, w.shape[1]
    m, n = tokens // 2, ff // 4

    def compute(step, ins, outs, _):
        outs[0][...] = dot(ins[0][...], ins[1][...], 1, 0)

    return run(
        number, 8, compute,
        [(a, pl.BlockSpec((m, d), lambda i: (i // 4, 0))), (w, pl.BlockSpec((d, n), lambda i: (0, i % 4)))],
        [(shape(tokens, ff, F32), pl.BlockSpec((m, n), lambda i: (i // 4, i % 4)))],
        comms,
    )


def k_up(number, a, w, gate, comms):
    (tokens, d), ff = a.shape, w.shape[1]
    m, n = tokens // 2, ff // 4
    tile = pl.BlockSpec((m, n), lambda i: (i // 4, i % 4))

    def compute(step, ins, outs, _):
        up = dot(ins[0][...], ins[1][...], 1, 0)
        outs[0][...] = up
        outs[1][...] = (jax.nn.silu(ins[2][...]) * up).astype(BF16)

    return run(
        number, 8, compute,
        [(a, pl.BlockSpec((m, d), lambda i: (i // 4, 0))), (w, pl.BlockSpec((d, n), lambda i: (0, i % 4))), (gate, tile)],
        [(shape(tokens, ff, F32), tile), (shape(tokens, ff), tile)],
        comms,
    )


def k_down(number, s, w, h, comms):
    (tokens, ff), d = s.shape, w.shape[1]
    m = tokens // 4
    rows = pl.BlockSpec((m, d), lambda i: (i, 0))

    def compute(step, ins, outs, scratch):
        choose(step, scratch[0])
        new = ins[2][...] + dot(ins[0][...], ins[1][...], 1, 0).astype(BF16)
        a = norm_rows(new.astype(F32))[1]
        outs[0][...] = new
        outs[1][...] = a
        outs[2][...] = dot(a, scratch[0][...], 1, 0).astype(BF16)

    return run(
        number, 4, compute,
        [(s, pl.BlockSpec((m, ff), lambda i: (i, 0))), (w, pl.BlockSpec((ff, d), lambda i: (0, 0), pipeline_mode=pl.Buffered(1))), (h, rows)],
        [(shape(tokens, d), rows)] * 3,
        comms,
        [pltpu.VMEM((d, d), BF16)],
    )


def exchange_scratch(n, rows, cols):
    return [pltpu.VMEM((n, rows, cols), BF16)] * 2 + [pltpu.SemaphoreType.DMA((n,))] * 2


def exchange(step, n, product, scratch, write):
    made, came, send, receive = scratch

    def copy(i):
        return remote(made.at[i], came.at[i], send.at[i], receive.at[i], C)

    for i in range(n):
        pl.when(step == i + 1)(lambda i=i: copy(i).start())
    total = product()

    @pl.when(step < n)
    def _():
        made[step] = total.astype(BF16)

    for i in range(n):

        @pl.when(step == i + n)
        def _(i=i):
            copy(i).wait_recv()
            write(i, total + came[i].astype(F32))
            if i == n - 1:
                for k in range(n):
                    copy(k).wait_send()


def k_gradient_in(number, a_split, d_gate, comms, sides=()):
    (tokens, d), ff = a_split.shape, d_gate.shape[1]
    rows, n = d // 8, ff // 4
    out = pl.BlockSpec((2 * rows, n), lambda i: (0, jnp.maximum(i - 4, 0)))

    def compute(step, ins, outs, scratch):
        def write(i, total):
            self, y, x, xy = (total[k * rows : (k + 1) * rows] for k in range(4))
            near, far = (x, y) if i < 2 else (y, x)
            outs[0][:rows, :] = near.astype(BF16)
            outs[0][rows:, :] = xy.astype(BF16)
            outs[1][:rows, :] = self
            outs[1][rows:, :] = far

        exchange(step, 4, lambda: dot(ins[0][...], ins[1][...], 0, 0), scratch, write)

    return run(
        number, 8, compute,
        [(a_split, pl.BlockSpec((tokens, d // 2), lambda i: (0, i // 4))), (d_gate, pl.BlockSpec((tokens, n), lambda i: (0, i % 4)))],
        [(shape(2 * rows, ff), out), (shape(2 * rows, ff, F32), out)],
        comms,
        exchange_scratch(4, 4 * rows, n),
        sides=sides,
    )


def k_gradient_down(number, s, d_out, comms, sides=()):
    (tokens, ff), d = s.shape, d_out.shape[1]
    rows, half = ff // 8, d // 2
    whole = pl.BlockSpec((2 * rows, d), lambda i: (0, 0), pipeline_mode=pl.Buffered(1))

    def block(i):
        return 0, place((i // 2 % 2, i % 2, 1 - i // 4))

    def compute(step, ins, outs, scratch):
        send, keep = outs

        def write(i, total):
            if i == 0:
                keep[:rows, :] = total
            elif i == 1:
                keep[rows:, :half] = total[:, :half]
                send[:rows, half:] = total[:, half:].astype(BF16)
            elif i == 2:
                send[:rows, :half] = total[:, :half].astype(BF16)
                keep[rows:, half:] = total[:, half:]
            else:
                send[rows:, :] = total.astype(BF16)

        exchange(step, 4, lambda: dot(ins[0][...], ins[1][...], 0, 0), scratch, write)

    return run(
        number, 8, compute,
        [(s, pl.BlockSpec((tokens, rows), block)), (d_out, pl.BlockSpec((tokens, d), lambda i: (0, 0), pipeline_mode=pl.Buffered(1)))],
        [(shape(2 * rows, d), whole), (shape(2 * rows, d, F32), whole)],
        comms,
        exchange_scratch(4, rows, d),
        sides=sides,
    )


def k_back_gated(number, d_out, w, gate, up, comms, sides=()):
    (tokens, d), ff = d_out.shape, w.shape[0]
    m, n = tokens // 2, ff // 4
    tile = pl.BlockSpec((m, n), lambda i: (i // 4, i % 4))

    def compute(step, ins, outs, _):
        ds = dot(ins[0][...], ins[1][...], 1, 1).astype(BF16).astype(F32)
        g, u = ins[2][...], ins[3][...]
        sig = jax.nn.sigmoid(g)
        acted = g * sig
        outs[0][...] = (ds * u * (sig * (1 + (g - acted)))).astype(BF16)
        outs[1][...] = (ds * acted).astype(BF16)

    return run(
        number, 8, compute,
        [(d_out, pl.BlockSpec((m, d), lambda i: (i // 4, 0))), (w, pl.BlockSpec((n, d), lambda i: (i % 4, 0))), (gate, tile), (up, tile)],
        [(shape(tokens, ff), tile), (shape(tokens, ff), tile)],
        comms,
        sides=sides,
    )


def k_back_norm(number, d_gate, w_gate, d_up, w_up, h, d_out, comms, sides=()):
    (tokens, ff), d = d_up.shape, w_up.shape[0]
    m = tokens // 8
    rows = pl.BlockSpec((m, d), lambda i: (i, 0))
    wide_rows = pl.BlockSpec((m, ff), lambda i: (i, 0))
    matrix = pl.BlockSpec((d, ff), lambda i: (0, 0), pipeline_mode=pl.Buffered(1))

    def compute(step, ins, outs, _):
        da = dot(ins[0][...], ins[1][...], 1, 1).astype(BF16)
        da = (da + dot(ins[2][...], ins[3][...], 1, 1).astype(BF16)).astype(F32)
        wide = ins[4][...].astype(F32)
        scale, _ = norm_rows(wide)
        inner = jnp.sum(da * wide, -1, keepdims=True) / d
        dh = da * scale - wide * (scale * scale * scale * inner)
        outs[0][...] = ins[5][...] + dh.astype(BF16)

    return run(
        number, 8, compute,
        [(d_gate, wide_rows), (w_gate, matrix), (d_up, wide_rows), (w_up, matrix), (h, rows), (d_out, rows)],
        [(shape(tokens, d), rows)],
        comms,
        sides=sides,
    )


def k_tail(number, u_send, u_keep, d_got, d_keep, g_got, g_keep, squares):
    (rows2, cols), (d_rows, d_cols) = u_keep.shape, d_keep.shape
    rows, half, quarter = rows2 // 2, cols // 2, cols // 4
    others = [(i // 4, i // 2 % 2, i % 2) for i in range(1, 8)]

    def kernel(*refs):
        u_s, u_k, d_g, d_k, g_g, g_k, sq_in, u_out, d_out, g_out, sq_out = refs[:11]
        uk, uc, u2, uc2, dk, dc, gk, gg, g2, gc, slots, mine, local, send, receive = refs[11:]
        barrier = pltpu.get_barrier_semaphore()
        for flip in others:
            pl.semaphore_signal(barrier, inc=1, device_id={"dp": place(flip)}, device_id_type=MESH)
        pl.semaphore_wait(barrier, len(others))

        def copy(i, src, dst, flip):
            return remote(src, dst, send.at[i], receive.at[i], flip)

        def part(ref, i, n):
            size = ref.shape[1] // n
            return ref.at[:, pl.ds(i * size, size)]

        first = [copy(i, part(u_s, i, 4), part(uc, i, 4), X if i < 2 else Y) for i in range(4)]
        g_hop = [copy(4 + i, part(g2, i, 2), part(gc, i, 2), (Y, X)[i]) for i in range(2)]
        second = [copy(6 + i, part(u2, i, 4), part(uc2, i, 4), Y if i < 2 else X) for i in range(4)]
        for i in (0, 2, 1, 3):
            first[i].start()
        loads = [pltpu.make_async_copy(s, t, local.at[i]) for i, (s, t) in enumerate(((g_k, gk), (g_g, gg), (u_k, uk), (d_k, dk), (d_g, dc)))]
        for one in loads:
            one.start()
        loads[0].wait()
        loads[1].wait()
        g2[...] = (gk[rows:, :] + gg[rows:, :].astype(F32)).astype(BF16)
        gk[:rows, :] = gk[:rows, :] + gg[:rows, :].astype(F32)
        for one in g_hop:
            one.start()
        loads[2].wait()
        for i in (0, 2, 1, 3):
            at = pl.ds(i * quarter, quarter)
            first[i].wait_recv()
            u2[:, at] = (uk[rows:, at] + uc[rows:, at].astype(F32)).astype(BF16)
            uk[:rows, at] = uk[:rows, at] + uc[:rows, at].astype(F32)
            second[i].start()

        total = sq_in[...]

        def final(out, keep, came, at):
            g = (keep[: came.shape[0], at] + came[:, at].astype(F32)).astype(BF16)
            out[:, at] = g
            wide = g.astype(F32)
            wide = jnp.sum((wide * wide).reshape(-1, 8, wide.shape[1]), 0)
            return sum(wide[:, k : k + 128] for k in range(0, wide.shape[1], 128))

        loads[3].wait()
        loads[4].wait()
        total += final(d_out, dk, dc, pl.ds(0, d_cols))
        for i in range(2):
            g_hop[i].wait_recv()
            total += final(g_out, gk, gc, pl.ds(i * half, half))
        for i in (0, 2, 1, 3):
            second[i].wait_recv()
            total += final(u_out, uk, uc2, pl.ds(i * quarter, quarter))
        mine[...] = total
        me = place((0, 0, 0))
        spread = [copy(10 + i, mine, slots.at[me], flip) for i, flip in enumerate(others)]
        for one in spread:
            one.start()
        slots[me] = total
        for one in spread:
            one.wait_recv()
        sq_out[...] = sum(slots[i] for i in range(8))
        for one in first + g_hop + second + spread:
            one.wait_send()

    vmem = pl.BlockSpec(memory_space=pltpu.VMEM)
    return pl.pallas_call(
        kernel,
        in_specs=[ANY] * 6 + [vmem],
        out_specs=[vmem] * 4,
        out_shape=[shape(rows, cols), shape(d_rows, d_cols), shape(rows, cols), shape(8, 128, F32)],
        scratch_shapes=[
            pltpu.VMEM((rows2, cols), F32), pltpu.VMEM((rows2, cols), BF16), pltpu.VMEM((rows, cols), BF16), pltpu.VMEM((rows, cols), BF16),
            pltpu.VMEM((d_rows, d_cols), F32), pltpu.VMEM((d_rows, d_cols), BF16),
            pltpu.VMEM((rows2, cols), F32), pltpu.VMEM((rows2, cols), BF16), pltpu.VMEM((rows, cols), BF16), pltpu.VMEM((rows, cols), BF16),
            pltpu.VMEM((8, 8, 128), F32), pltpu.VMEM((8, 128), F32),
            pltpu.SemaphoreType.DMA((5,)), pltpu.SemaphoreType.DMA((17,)), pltpu.SemaphoreType.DMA((17,)),
        ],
        compiler_params=pltpu.CompilerParams(collective_id=number, has_side_effects=True, vmem_limit_bytes=VMEM_LIMIT),
        cost_estimate=pl.CostEstimate(flops=10**9, bytes_accessed=5 * 10**7, transcendentals=0),
        name=f"k{number}",
    )(u_send, u_keep, d_got, d_keep, g_got, g_keep, squares)


def adamw(w, m, v, g):
    m = 0.9 * m + 0.1 * g
    v = 0.95 * v + 0.05 * g * g
    step = m * lax.rsqrt(v + 1e-8) + 0.1 * w
    return (w - 0.02 * step).astype(BF16), m, v


def solution(mesh):
    def step(x, dy, *arrays):
        weights, ms, vs = (arrays[i : i + 3] for i in (0, 3, 6))
        h0, dy = x[0], dy[0]
        (g0, g1), (u0, u1), (d0, d1) = ((w[0], w[1]) for w in weights)

        a0, a0s, wg0 = k_norm(0, h0, [Gather(g0, 1)])
        gate0, wu0 = k_gate(1, a0, wg0, [Gather(u0, 4)])
        up0, s0, wd0 = k_up(2, a0, wu0, gate0, [Gather(d0, 4)])
        h1, a1, a1s, wg1 = k_down(3, s0, wd0, h0, [Gather(g1, 2)])
        gate1, wu1 = k_gate(4, a1, wg1, [Gather(u1, 4)])
        up1, s1, wd1 = k_up(5, a1, wu1, gate1, [Gather(d1, 4)])

        done, total = {}, 0.0
        d1_send, d1_keep = k_gradient_down(6, s1, dy, [])
        dgate1, dup1, got = k_back_gated(7, dy, wd1, gate1, up1, [Hop(d1_send, X, Y)])
        g1_send, g1_keep, d1_keep, got_d = k_gradient_in(8, a1s, dgate1, [AddHop(d1_keep, got, Y, X, 1)])
        u1_send, u1_keep, got = k_gradient_in(9, a1s, dup1, [Hop(g1_send, X, Y)])
        dh1, done["d1"], sums, g1_keep, got_g, got = k_back_norm(
            10, dgate1, wg1, dup1, wu1, h1, dy, [AddHop(g1_keep, got, Y, X, 1), Hop(u1_send, X, Y)], [side_last(d1_keep, got_d)]
        )
        total += jnp.sum(sums)
        d0_send, d0_keep, done["g1"], sums, u1_keep, got_u = k_gradient_down(
            11, s0, dh1, [AddHop(u1_keep, got, Y, X, 1)], [side_last(g1_keep, got_g)]
        )
        total += jnp.sum(sums)
        dgate0, dup0, done["u1"], sums, got = k_back_gated(12, dh1, wd0, gate0, up0, [Hop(d0_send, X, Y)], [side_last(u1_keep, got_u)])
        total += jnp.sum(sums)
        g0_send, g0_keep, d0_keep, got_d = k_gradient_in(13, a0s, dgate0, [AddHop(d0_keep, got, Y, X, 1)])
        u0_send, u0_keep, got = k_gradient_in(14, a0s, dup0, [Hop(g0_send, X, Y)])
        squares = jnp.zeros((8, 128), F32).at[0, 0].set(total)
        done["u0"], done["d0"], done["g0"], squares = k_tail(15, u0_send, u0_keep, got_d, d0_keep, got, g0_keep, squares)
        total = jnp.sum(squares)
        count = 8 * sum(g.size for g in done.values())
        factor = jnp.minimum(1.0, 0.5 * lax.rsqrt(total / count + 1e-30))
        new = []
        for i, name in enumerate("gud"):
            g = jnp.stack([done[name + "0"], done[name + "1"]]).astype(F32) * factor
            new.append(adamw(weights[i].astype(F32), ms[i], vs[i], g))
        return tuple(one[which] for which in range(3) for one in new)

    states, cut = P(("rep", "dp"), None, None), P(None, "dp", None)
    return jax.shard_map(
        step,
        mesh=mesh,
        in_specs=(states, states) + (cut,) * 9,
        out_specs=(P("rep", "dp", None),) * 9,
        check_vma=False,
    )
```

```python
import jax
import jax.numpy as jnp
from jax import lax
from jax.experimental import pallas as pl
from jax.experimental.pallas import tpu as pltpu
from jax.sharding import PartitionSpec as P

F32, BF16 = jnp.float32, jnp.bfloat16
X, Y, C = (1, 0, 0), (0, 1, 0), (0, 0, 1)
DIAGONAL = (1, 1, 0)
MESH = pl.DeviceIdType.MESH
ALL = ...
COST = pl.CostEstimate(flops=10**9, bytes_accessed=5 * 10**7, transcendentals=0)
ANY = pl.BlockSpec(memory_space=pl.ANY)
VMEM_LIMIT = 63 * 2**20


def dot(a, b, ca, cb):
    return lax.dot_general(a, b, (((ca,), (cb,)), ((), ())), preferred_element_type=F32)


def place(flip):
    index = lax.axis_index("dp")
    x, y, core = index // 4, index // 2 % 2, index % 2
    return (x + flip[0]) % 2 * 4 + (y + flip[1]) % 2 * 2 + (core + flip[2]) % 2


def remote(src, dst, send, receive, flip):
    return pltpu.make_async_remote_copy(
        src_ref=src, dst_ref=dst, send_sem=send, recv_sem=receive, device_id={"dp": place(flip)}, device_id_type=MESH
    )


def greet():
    barrier = pltpu.get_barrier_semaphore()
    for flip in (X, Y, C):
        pl.semaphore_signal(barrier, inc=1, device_id={"dp": place(flip)}, device_id_type=MESH)
    pl.semaphore_wait(barrier, 3)


class Gather:
    def __init__(self, w, layer, middle, rest=True):
        self.inputs, self.middle, self.layer, self.rest = [w.reshape(-1, w.shape[2])], middle, layer, rest
        _, self.rows, cols = w.shape
        self.outputs = [jax.ShapeDtypeStruct((8 * self.rows, cols), BF16)]
        self.scratch = [pltpu.VMEM((self.rows, cols), BF16), pltpu.SemaphoreType.DMA((2,)), pltpu.SemaphoreType.DMA((17,)), pltpu.SemaphoreType.DMA((17,))]

    def bind(self, refs_in, refs_out, scratch):
        (w,), (self.full,), (held, local, self.send, self.receive) = refs_in, refs_out, scratch
        half, rows = self.rows // 2, self.rows
        self.shard = w.at[pl.ds(self.layer * rows, rows)]
        self.xa, self.xb = self.copy(0, X, None, 0, half), self.copy(1, X, None, half, half)
        self.yb, self.ya = self.copy(2, Y, None, half, half), self.copy(3, Y, None, 0, half)
        self.own = self.copy(4, C, None, 0, rows)
        self.cxa, self.cxb = self.copy(5, C, X, 0, half), self.copy(6, C, X, half, half)
        self.cyb, self.cya = self.copy(7, C, Y, half, half), self.copy(8, C, Y, 0, half)
        self.bind_rest(9)
        self.load = pltpu.make_async_copy(self.shard, held, local.at[0])
        self.store = pltpu.make_async_copy(held, self.part((0, 0, 0), 0, rows), local.at[1])

    def part(self, flip, first, count):
        return self.full.at[pl.ds(pl.multiple_of(place(flip) * self.rows, 8) + first, count)]

    def copy(self, number, flip, of, first, count):
        src = self.shard.at[pl.ds(first, count)] if of is None else self.part(of, first, count)
        return remote(src, self.part(of or (0, 0, 0), first, count), self.send.at[number], self.receive.at[number], flip)

    def bind_rest(self, number):
        q = self.rows // 4
        self.far = [self.copy(number + i, (Y, X)[i % 2], (X, Y)[i % 2], (i % 2 * 2 + i // 2) * q, q) for i in range(4)]
        self.across = [self.copy(number + 4 + i, C, DIAGONAL, (i % 2 * 2 + i // 2) * q, q) for i in range(4)]

    def start(self):
        for one in (self.xa, self.yb, self.xb, self.ya, self.own, self.load):
            one.start()

    def relay(self):
        self.xa.wait_recv()
        if self.rest:
            self.far[0].start()
            self.far[2].start()
        self.cxa.start()
        self.yb.wait_recv()
        if self.rest:
            self.far[1].start()
            self.far[3].start()
        self.cyb.start()
        self.load.wait()
        self.store.start()

    def finish_rest(self):
        for far, across in zip(self.far, self.across):
            far.wait_recv()
            across.start()

    def wait_rest(self):
        for one in self.across:
            one.wait_recv()
        for one in self.far + self.across:
            one.wait_send()

    def finish(self):
        self.xb.wait_recv()
        self.cxb.start()
        self.ya.wait_recv()
        self.cya.start()
        if self.rest:
            self.finish_rest()
        for one in (self.own, self.cxa, self.cyb, self.cxb, self.cya):
            one.wait_recv()
        for one in (self.xa, self.xb, self.yb, self.ya, self.own, self.cxa, self.cyb, self.cxb, self.cya):
            one.wait_send()
        if self.rest:
            self.wait_rest()
        self.store.wait()


class GatherRest(Gather):
    def __init__(self, full, middle):
        self.inputs, self.middle, self.rows = [full], middle, full.shape[0] // 8
        self.outputs = [jax.ShapeDtypeStruct(full.shape, BF16)]
        self.scratch = [pltpu.SemaphoreType.DMA((8,)), pltpu.SemaphoreType.DMA((8,))]

    def bind(self, refs_in, refs_out, scratch):
        (self.full,), (self.send, self.receive) = refs_out, scratch
        self.bind_rest(0)

    def start(self):
        for one in self.far:
            one.start()

    def relay(self):
        self.finish_rest()

    def finish(self):
        self.wait_rest()


class Hop:
    def __init__(self, array, left, right):
        self.inputs, self.flips, self.middle = [array], (left, right), None
        self.outputs = [jax.ShapeDtypeStruct(array.shape, array.dtype)]
        self.scratch = [pltpu.SemaphoreType.DMA((2,)), pltpu.SemaphoreType.DMA((2,))]

    def bind(self, refs_in, refs_out, scratch):
        (src,), (dst,), (send, receive) = refs_in, refs_out, scratch
        half = src.shape[1] // 2
        self.copies = [
            remote(src.at[:, pl.ds(i * half, half)], dst.at[:, pl.ds(i * half, half)], send.at[i], receive.at[i], flip)
            for i, flip in enumerate(self.flips)
        ]

    def start(self):
        for one in self.copies:
            one.start()

    def finish(self):
        for one in self.copies:
            one.wait_recv()
        for one in self.copies:
            one.wait_send()


class AddHop:
    def __init__(self, keep, got, left, right, middle):
        self.inputs, self.flips, self.middle = [keep, got], (left, right), middle
        rows, cols = keep.shape[0] // 2, keep.shape[1]
        self.outputs = [jax.ShapeDtypeStruct((rows, cols), F32), jax.ShapeDtypeStruct((rows, cols), BF16)]
        self.scratch = [pltpu.VMEM(keep.shape, F32), pltpu.VMEM(got.shape, BF16), pltpu.VMEM((rows, cols), BF16), pltpu.SemaphoreType.DMA((3,))]
        self.scratch += [pltpu.SemaphoreType.DMA((2,)), pltpu.SemaphoreType.DMA((2,))]

    def bind(self, refs_in, refs_out, scratch):
        (keep, got), (stay, dst), (self.sum, self.came, self.out, local, send, receive) = refs_in, refs_out, scratch
        self.rows, half = dst.shape[0], dst.shape[1] // 2
        self.loads = [pltpu.make_async_copy(keep, self.sum, local.at[0]), pltpu.make_async_copy(got, self.came, local.at[1])]
        self.store = pltpu.make_async_copy(self.sum.at[pl.ds(0, self.rows)], stay, local.at[2])
        self.copies = [
            remote(self.out.at[:, pl.ds(i * half, half)], dst.at[:, pl.ds(i * half, half)], send.at[i], receive.at[i], flip)
            for i, flip in enumerate(self.flips)
        ]

    def start(self):
        for one in self.loads:
            one.start()

    def relay(self):
        for one in self.loads:
            one.wait()
        rows = self.rows
        self.out[ALL] = (self.sum[rows:, :] + self.came[rows:, :].astype(F32)).astype(BF16)
        self.sum[:rows, :] = self.sum[:rows, :] + self.came[:rows, :].astype(F32)
        self.store.start()
        for one in self.copies:
            one.start()

    def finish(self):
        for one in self.copies:
            one.wait_recv()
        for one in self.copies:
            one.wait_send()
        self.store.wait()


def run(number, steps, compute, ins, outs, comms, scratch=(), sides=()):
    sides = [side(steps) for side in sides]
    counts = [len(ins)] + [len(s[0]) for s in sides] + [len(c.inputs) for c in comms]
    counts += [len(outs)] + [len(s[1]) for s in sides] + [len(c.outputs) for c in comms]
    counts += [len(scratch)] + [len(c.scratch) for c in comms]

    def kernel(*refs):
        refs, groups = list(refs), []
        for count in counts:
            groups.append(refs[:count])
            refs = refs[count:]
        n, k = len(sides), len(sides) + len(comms) + 1
        g_in, g_out, g_scratch = groups[:k], groups[k : 2 * k], groups[2 * k :]
        for c, *bound in zip(comms, g_in[1 + n :], g_out[1 + n :], g_scratch[1:]):
            c.bind(*bound)
        step = pl.program_id(0)

        @pl.when(step == 0)
        def _():
            greet()
            for c in comms:
                c.start()

        for c in comms:
            if c.middle is not None:
                pl.when(step == c.middle)(c.relay)
        if compute is not None:
            compute(step, g_in[0], g_out[0], g_scratch[0])
        for s, s_in, s_out in zip(sides, g_in[1:], g_out[1:]):
            s[2](s_in, s_out)

        @pl.when(step == steps - 1)
        def _():
            for c in comms:
                c.finish()

    ins = list(ins) + [one for s in sides for one in s[0]]
    outs = list(outs) + [one for s in sides for one in s[1]]
    at_in, at_out, aliases = len(ins), len(outs), {}
    for c in comms:
        if isinstance(c, GatherRest):
            aliases[at_in] = at_out
        at_in, at_out = at_in + len(c.inputs), at_out + len(c.outputs)
    return pl.pallas_call(
        kernel,
        grid=(steps,),
        input_output_aliases=aliases,
        in_specs=[spec for _, spec in ins] + [ANY for c in comms for _ in c.inputs],
        out_specs=[spec for _, spec in outs] + [ANY for c in comms for _ in c.outputs],
        out_shape=[shape for shape, _ in outs] + [shape for c in comms for shape in c.outputs],
        scratch_shapes=list(scratch) + [s for c in comms for s in c.scratch],
        compiler_params=pltpu.CompilerParams(
            collective_id=number, has_side_effects=True, vmem_limit_bytes=VMEM_LIMIT, dimension_semantics=("arbitrary",)
        ),
        cost_estimate=COST,
        name=f"k{number}",
    )(*[a for a, _ in ins], *[a for c in comms for a in c.inputs])


def blocks(rows, cols, steps):
    n = min(steps, 8)
    per = steps // n
    if rows % (16 * n) == 0:
        return tuple(pl.BlockSpec((rows // n, cols), lambda i, k=k: (i // per + k * n, 0)) for k in (0, 1)) + (n, pl.BlockSpec((8, cols), lambda i: (i // per, 0)))
    return tuple(pl.BlockSpec((rows, cols // n), lambda i, k=k: (k, i // per)) for k in (0, 1)) + (1, pl.BlockSpec((8, cols // n), lambda i: (0, i // per)))


def side_last(keep, got):
    rows, cols = keep.shape

    def side(steps):
        low, _, n, sums = blocks(rows, cols, steps)

        def compute(ins, outs):
            g = (ins[0][ALL] + ins[1][ALL].astype(F32)).astype(BF16)
            outs[0][ALL] = g
            wide = g.astype(F32)
            outs[1][ALL] = jnp.sum((wide * wide).reshape(-1, 8, wide.shape[1]), 0)

        return [(keep, low), (got, low)], [(shape(rows, cols), low), (shape(8 * n, cols, F32), sums)], compute

    return side


def shape(rows, cols, dtype=BF16):
    return jax.ShapeDtypeStruct((rows, cols), dtype)


def norm_rows(wide):
    scale = lax.rsqrt(jnp.mean(wide * wide, -1, keepdims=True) + 1e-6)
    return scale, (wide * scale).astype(BF16)


def choose(step, chosen):
    width = chosen.shape[1] // 8

    @pl.when(step == 0)
    def _():
        away = lax.broadcasted_iota(jnp.int32, (chosen.shape[0], width), 0) - lax.broadcasted_iota(jnp.int32, (chosen.shape[0], width), 1)
        for i in range(8):
            chosen[:, i * width : (i + 1) * width] = jnp.where(away == place((i // 2 % 2, i % 2, 1 - i // 4)) * width, 1.0, 0.0).astype(BF16)


def k_norm(number, h, comms):
    tokens, d = h.shape
    rows = tokens // 4
    block = pl.BlockSpec((rows, d), lambda i: (i, 0))

    def compute(step, ins, outs, scratch):
        choose(step, scratch[0])
        a = norm_rows(ins[0][ALL].astype(F32))[1]
        outs[0][ALL] = a
        outs[1][ALL] = dot(a, scratch[0][ALL], 1, 0).astype(BF16)

    return run(number, 4, compute, [(h, block)], [(shape(tokens, d), block)] * 2, comms, [pltpu.VMEM((d, d), BF16)])


def k_gate(number, a, w, comms):
    (tokens, d), ff = a.shape, w.shape[1]
    m, n = tokens // 2, ff // 4

    def compute(step, ins, outs, _):
        outs[0][ALL] = dot(ins[0][ALL], ins[1][ALL], 1, 0)

    return run(
        number, 8, compute,
        [(a, pl.BlockSpec((m, d), lambda i: (i // 4, 0))), (w, pl.BlockSpec((d, n), lambda i: (0, i % 4)))],
        [(shape(tokens, ff, F32), pl.BlockSpec((m, n), lambda i: (i // 4, i % 4)))],
        comms,
    )


def k_up(number, a, w, gate, comms):
    (tokens, d), ff = a.shape, w.shape[1]
    m, n = tokens // 2, ff // 4
    tile = pl.BlockSpec((m, n), lambda i: (i // 4, i % 4))

    def compute(step, ins, outs, _):
        up = dot(ins[0][ALL], ins[1][ALL], 1, 0)
        outs[0][ALL] = up
        outs[1][ALL] = (jax.nn.silu(ins[2][ALL]) * up).astype(BF16)

    return run(
        number, 8, compute,
        [(a, pl.BlockSpec((m, d), lambda i: (i // 4, 0))), (w, pl.BlockSpec((d, n), lambda i: (0, i % 4))), (gate, tile)],
        [(shape(tokens, ff, F32), tile), (shape(tokens, ff), tile)],
        comms,
    )


def k_down(number, s, w, h, comms):
    (tokens, ff), d = s.shape, w.shape[1]
    m = tokens // 4
    rows = pl.BlockSpec((m, d), lambda i: (i, 0))

    def compute(step, ins, outs, scratch):
        held, sem = scratch[1:]

        @pl.when(step == 0)
        def _():
            pltpu.make_async_copy(ins[1], held, sem).start()

        choose(step, scratch[0])

        @pl.when(step == 0)
        def _():
            pltpu.make_async_copy(ins[1], held, sem).wait()

        new = ins[2][ALL] + dot(ins[0][ALL], held[ALL], 1, 0).astype(BF16)
        a = norm_rows(new.astype(F32))[1]
        outs[0][ALL] = new
        outs[1][ALL] = a
        outs[2][ALL] = dot(a, scratch[0][ALL], 1, 0).astype(BF16)

    return run(
        number, 4, compute,
        [(s, pl.BlockSpec((m, ff), lambda i: (i, 0))), (w, ANY), (h, rows)],
        [(shape(tokens, d), rows)] * 3,
        comms,
        [pltpu.VMEM((d, d), BF16), pltpu.VMEM((ff, d), BF16), pltpu.SemaphoreType.DMA],
    )


def exchange_scratch(n, rows, cols):
    return [pltpu.VMEM((n, rows, cols), BF16)] * 2 + [pltpu.SemaphoreType.DMA((n,))] * 2


def exchange(step, n, product, scratch, write):
    made, came, send, receive = scratch

    def copy(i):
        return remote(made.at[i], came.at[i], send.at[i], receive.at[i], C)

    for i in range(n):
        pl.when(step == i + 1)(lambda i=i: copy(i).start())
    total = product()

    @pl.when(step < n)
    def _():
        made[step] = total.astype(BF16)

    for i in range(n):

        @pl.when(step == i + n)
        def _(i=i):
            copy(i).wait_recv()
            write(i, total + came[i].astype(F32))
            if i == n - 1:
                for k in range(n):
                    copy(k).wait_send()


def k_gradient_in(number, a_split, d_gate, comms, sides=()):
    (tokens, d), ff = a_split.shape, d_gate.shape[1]
    rows, n = d // 8, ff // 4
    out = pl.BlockSpec((2 * rows, n), lambda i: (0, jnp.maximum(i - 4, 0)))

    def compute(step, ins, outs, scratch):
        def write(i, total):
            self, y, x, xy = (total[k * rows : (k + 1) * rows] for k in range(4))
            near, far = (x, y) if i < 2 else (y, x)
            outs[0][:rows, :] = near.astype(BF16)
            outs[0][rows:, :] = xy.astype(BF16)
            outs[1][:rows, :] = self
            outs[1][rows:, :] = far

        exchange(step, 4, lambda: dot(ins[0][ALL], ins[1][ALL], 0, 0), scratch, write)

    return run(
        number, 8, compute,
        [(a_split, pl.BlockSpec((tokens, d // 2), lambda i: (0, i // 4))), (d_gate, pl.BlockSpec((tokens, n), lambda i: (0, i % 4)))],
        [(shape(2 * rows, ff), out), (shape(2 * rows, ff, F32), out)],
        comms,
        exchange_scratch(4, 4 * rows, n),
        sides=sides,
    )


def k_gradient_down(number, s, d_out, comms, sides=()):
    (tokens, ff), d = s.shape, d_out.shape[1]
    rows, half = ff // 8, d // 2
    whole = pl.BlockSpec((2 * rows, d), lambda i: (0, 0), pipeline_mode=pl.Buffered(1))

    def block(i):
        return 0, place((i // 2 % 2, i % 2, 1 - i // 4))

    def compute(step, ins, outs, scratch):
        send, keep = outs

        def write(i, total):
            if i == 0:
                keep[:rows, :] = total
            elif i == 1:
                keep[rows:, :half] = total[:, :half]
                send[:rows, half:] = total[:, half:].astype(BF16)
            elif i == 2:
                send[:rows, :half] = total[:, :half].astype(BF16)
                keep[rows:, half:] = total[:, half:]
            else:
                send[rows:, :] = total.astype(BF16)

        exchange(step, 4, lambda: dot(ins[0][ALL], ins[1][ALL], 0, 0), scratch, write)

    return run(
        number, 8, compute,
        [(s, pl.BlockSpec((tokens, rows), block)), (d_out, pl.BlockSpec((tokens, d), lambda i: (0, 0), pipeline_mode=pl.Buffered(1)))],
        [(shape(2 * rows, d), whole), (shape(2 * rows, d, F32), whole)],
        comms,
        exchange_scratch(4, rows, d),
        sides=sides,
    )


def k_back_gated(number, d_out, w, gate, up, comms, sides=()):
    (tokens, d), ff = d_out.shape, w.shape[0]
    m, n = tokens // 2, ff // 4
    tile = pl.BlockSpec((m, n), lambda i: (i // 4, i % 4))

    def compute(step, ins, outs, _):
        ds = dot(ins[0][ALL], ins[1][ALL], 1, 1).astype(BF16).astype(F32)
        g, u = ins[2][ALL], ins[3][ALL]
        sig = jax.nn.sigmoid(g)
        acted = g * sig
        outs[0][ALL] = (ds * u * (sig * (1 + (g - acted)))).astype(BF16)
        outs[1][ALL] = (ds * acted).astype(BF16)

    return run(
        number, 8, compute,
        [(d_out, pl.BlockSpec((m, d), lambda i: (i // 4, 0))), (w, pl.BlockSpec((n, d), lambda i: (i % 4, 0))), (gate, tile), (up, tile)],
        [(shape(tokens, ff), tile), (shape(tokens, ff), tile)],
        comms,
        sides=sides,
    )


def k_back_norm(number, d_gate, w_gate, d_up, w_up, h, d_out, comms, sides=()):
    (tokens, ff), d = d_up.shape, w_up.shape[0]
    m = tokens // 8
    rows = pl.BlockSpec((m, d), lambda i: (i, 0))
    wide_rows = pl.BlockSpec((m, ff), lambda i: (i, 0))
    matrix = pl.BlockSpec((d, ff), lambda i: (0, 0), pipeline_mode=pl.Buffered(1))

    def compute(step, ins, outs, _):
        da = dot(ins[0][ALL], ins[1][ALL], 1, 1).astype(BF16)
        da = (da + dot(ins[2][ALL], ins[3][ALL], 1, 1).astype(BF16)).astype(F32)
        wide = ins[4][ALL].astype(F32)
        scale, _ = norm_rows(wide)
        inner = jnp.sum(da * wide, -1, keepdims=True) / d
        dh = da * scale - wide * (scale * scale * scale * inner)
        outs[0][ALL] = ins[5][ALL] + dh.astype(BF16)

    return run(
        number, 8, compute,
        [(d_gate, wide_rows), (w_gate, matrix), (d_up, wide_rows), (w_up, matrix), (h, rows), (d_out, rows)],
        [(shape(tokens, d), rows)],
        comms,
        sides=sides,
    )


def k_tail(number, u_send, u_keep, d_got, d_keep, g_got, g_keep, sums):
    (rows2, cols), (d_rows, d_cols) = u_keep.shape, d_keep.shape
    rows, half, quarter = rows2 // 2, cols // 2, cols // 4
    others = [(i // 4, i // 2 % 2, i % 2) for i in range(1, 8)]

    def kernel(*refs):
        refs = list(refs)
        u_s, u_k, d_g, d_k, g_g, g_k = refs[:6]
        so_far, refs = refs[6 : 6 + len(sums)], refs[6 + len(sums) :]
        u_out, d_out, g_out, sq_out = refs[:4]
        uk, uc, u2, uc2, dk, dc, gk, gg, g2, gc, slots, mine, local, send, receive = refs[4:]
        barrier = pltpu.get_barrier_semaphore()
        for flip in others:
            pl.semaphore_signal(barrier, inc=1, device_id={"dp": place(flip)}, device_id_type=MESH)
        pl.semaphore_wait(barrier, len(others))

        def copy(i, src, dst, flip):
            return remote(src, dst, send.at[i], receive.at[i], flip)

        def part(ref, i, n):
            size = ref.shape[1] // n
            return ref.at[:, pl.ds(i * size, size)]

        first = [copy(i, part(u_s, i, 4), part(uc, i, 4), X if i < 2 else Y) for i in range(4)]
        g_hop = [copy(4 + i, part(g2, i, 2), part(gc, i, 2), (Y, X)[i]) for i in range(2)]
        second = [copy(6 + i, part(u2, i, 4), part(uc2, i, 4), Y if i < 2 else X) for i in range(4)]
        for i in (0, 2, 1, 3):
            first[i].start()
        loads = [pltpu.make_async_copy(s, t, local.at[i]) for i, (s, t) in enumerate(((g_k, gk), (g_g, gg), (u_k, uk), (d_k, dk), (d_g, dc)))]
        for one in loads:
            one.start()
        loads[0].wait()
        loads[1].wait()
        g2[ALL] = (gk[rows:, :] + gg[rows:, :].astype(F32)).astype(BF16)
        gk[:rows, :] = gk[:rows, :] + gg[:rows, :].astype(F32)
        for one in g_hop:
            one.start()
        loads[2].wait()
        for i in (0, 2, 1, 3):
            at = pl.ds(i * quarter, quarter)
            first[i].wait_recv()
            u2[:, at] = (uk[rows:, at] + uc[rows:, at].astype(F32)).astype(BF16)
            uk[:rows, at] = uk[:rows, at] + uc[:rows, at].astype(F32)
            second[i].start()

        def folded(wide):
            wide = jnp.sum(wide.reshape(-1, 8, wide.shape[1]), 0)
            return sum(wide[:, k : k + 128] for k in range(0, wide.shape[1], 128))

        total = sum(folded(one[ALL]) for one in so_far)

        def final(out, keep, came, at):
            g = (keep[: came.shape[0], at] + came[:, at].astype(F32)).astype(BF16)
            out[:, at] = g
            wide = g.astype(F32)
            return folded(wide * wide)

        loads[3].wait()
        loads[4].wait()
        total += final(d_out, dk, dc, pl.ds(0, d_cols))
        for i in range(2):
            g_hop[i].wait_recv()
            total += final(g_out, gk, gc, pl.ds(i * half, half))
        for i in (0, 2, 1, 3):
            second[i].wait_recv()
            total += final(u_out, uk, uc2, pl.ds(i * quarter, quarter))
        mine[ALL] = total
        me = place((0, 0, 0))
        spread = [copy(10 + i, mine, slots.at[me], flip) for i, flip in enumerate(others)]
        for one in spread:
            one.start()
        slots[me] = total
        for one in spread:
            one.wait_recv()
        sq_out[ALL] = sum(slots[i] for i in range(8))
        for one in first + g_hop + second + spread:
            one.wait_send()

    vmem = pl.BlockSpec(memory_space=pltpu.VMEM)
    return pl.pallas_call(
        kernel,
        in_specs=[ANY] * 6 + [vmem] * len(sums),
        out_specs=[vmem] * 4,
        out_shape=[shape(rows, cols), shape(d_rows, d_cols), shape(rows, cols), shape(8, 128, F32)],
        scratch_shapes=[
            pltpu.VMEM((rows2, cols), F32), pltpu.VMEM((rows2, cols), BF16), pltpu.VMEM((rows, cols), BF16), pltpu.VMEM((rows, cols), BF16),
            pltpu.VMEM((d_rows, d_cols), F32), pltpu.VMEM((d_rows, d_cols), BF16),
            pltpu.VMEM((rows2, cols), F32), pltpu.VMEM((rows2, cols), BF16), pltpu.VMEM((rows, cols), BF16), pltpu.VMEM((rows, cols), BF16),
            pltpu.VMEM((8, 8, 128), F32), pltpu.VMEM((8, 128), F32),
            pltpu.SemaphoreType.DMA((5,)), pltpu.SemaphoreType.DMA((17,)), pltpu.SemaphoreType.DMA((17,)),
        ],
        compiler_params=pltpu.CompilerParams(collective_id=number, has_side_effects=True, vmem_limit_bytes=VMEM_LIMIT),
        cost_estimate=COST,
        name=f"k{number}",
    )(u_send, u_keep, d_got, d_keep, g_got, g_keep, *sums)


def adamw(w, m, v, g):
    m = 0.9 * m + 0.1 * g
    v = 0.95 * v + 0.05 * g * g
    step = m * lax.rsqrt(v + 1e-8) + 0.1 * w
    return (w - 0.02 * step).astype(BF16), m, v


def solution(mesh):
    def step(x, dy, *arrays):
        weights, ms, vs = (arrays[i : i + 3] for i in (0, 3, 6))
        h0, dy = x[0], dy[0]
        gate, up, down = weights

        a0, a0s, wg0 = k_norm(0, h0, [Gather(gate, 0, 1)])
        gate0, wu0 = k_gate(1, a0, wg0, [Gather(up, 0, 4)])
        up0, s0, wd0 = k_up(2, a0, wu0, gate0, [Gather(down, 0, 4)])
        h1, a1, a1s, wg1 = k_down(3, s0, wd0, h0, [Gather(gate, 1, 2)])
        gate1, wu1 = k_gate(4, a1, wg1, [Gather(up, 1, 4)])
        up1, s1, wd1 = k_up(5, a1, wu1, gate1, [Gather(down, 1, 4, rest=False)])

        done = {}
        d1_send, d1_keep, wd1 = k_gradient_down(6, s1, dy, [GatherRest(wd1, 6)])
        dgate1, dup1, got = k_back_gated(7, dy, wd1, gate1, up1, [Hop(d1_send, X, Y)])
        g1_send, g1_keep, d1_keep, got_d = k_gradient_in(8, a1s, dgate1, [AddHop(d1_keep, got, Y, X, 1)])
        u1_send, u1_keep, got = k_gradient_in(9, a1s, dup1, [Hop(g1_send, X, Y)])
        dh1, done["d1"], sums_d, g1_keep, got_g, got = k_back_norm(
            10, dgate1, wg1, dup1, wu1, h1, dy, [AddHop(g1_keep, got, Y, X, 1), Hop(u1_send, X, Y)], [side_last(d1_keep, got_d)]
        )
        d0_send, d0_keep, done["g1"], sums_g, u1_keep, got_u = k_gradient_down(
            11, s0, dh1, [AddHop(u1_keep, got, Y, X, 1)], [side_last(g1_keep, got_g)]
        )
        dgate0, dup0, done["u1"], sums_u, got = k_back_gated(12, dh1, wd0, gate0, up0, [Hop(d0_send, X, Y)], [side_last(u1_keep, got_u)])
        g0_send, g0_keep, d0_keep, got_d = k_gradient_in(13, a0s, dgate0, [AddHop(d0_keep, got, Y, X, 1)])
        u0_send, u0_keep, got = k_gradient_in(14, a0s, dup0, [Hop(g0_send, X, Y)])
        done["u0"], done["d0"], done["g0"], squares = k_tail(15, u0_send, u0_keep, got_d, d0_keep, got, g0_keep, (sums_d, sums_g, sums_u))
        total = jnp.sum(squares)
        count = 8 * sum(g.size for g in done.values())
        factor = jnp.minimum(1.0, 0.5 * lax.rsqrt(total / count + 1e-30))
        new = []
        for i, name in enumerate("gud"):
            g = jnp.stack([done[name + "0"], done[name + "1"]]).astype(F32) * factor
            new.append(adamw(weights[i].astype(F32), ms[i], vs[i], g))
        return tuple(one[which] for which in range(3) for one in new)

    states, cut = P(("rep", "dp"), None, None), P(None, "dp", None)
    return jax.shard_map(
        step,
        mesh=mesh,
        in_specs=(states, states) + (cut,) * 9,
        out_specs=(P("rep", "dp", None),) * 9,
        check_vma=False,
    )
```
